32 devices in a mesh: seq: 16 (over z, y, core), grp: 2 (over x).
Axes of the slice: x: 2, y: 2, z: 4, core: 2. Of those that a mesh axis runs over, the one named last changes fastest.
Arguments:
- queries: bfloat16 [4096, 3584], P(('grp', 'seq')), parts along dimension 0, may hold values from -5 to 5
- keys: bfloat16 [4096, 512], P(('grp', 'seq')), parts along dimension 0, may hold values from -5 to 5
- values: bfloat16 [4096, 512], P(('grp', 'seq')), parts along dimension 0, may hold values from -6 to 6
- doc_lengths: int32 [16], P('grp'), parts along dimension 0, may hold values from 1 to 1280, 2048 in all
Outputs:
- attended: bfloat16 [4096, 3584], P(('grp', 'seq')), parts along dimension 0
The draws below stay inside these ranges and needn't reach their ends.
There are 2 independent parts, one for each index of `grp`. The reference program is written for one: setup_inputs(seed, part) draws one part's arguments, and reference() takes and returns one part's arrays. A program takes and returns all parts, laid end to end along the dimension named above; each array names one. Nothing has to cross between parts.
Inputs may be any that keep to these rules, and one draw needn't show every extreme that they name: `doc_lengths`: the 8 documents lie one after another and their lengths sum to 2048; the longest has exactly 1280 tokens.
All inputs are finite; a program needn't handle non-finite values.
Results may differ from the reference program's by a relative error of at most 0.0085.
Values may be sent and summed in bfloat16 or wider, within the bound.
A program may use at most 192 MiB of HBM per device.

```python
import math
import jax
import jax.numpy as jnp
import numpy as np
from jax import lax

HEADS = 28
KV_HEADS = 4
HEAD_DIM = 128
DOCS = 8
SEQ_LEN = 2048
MOST_DOC = 1280


def draw_keys(key, part):
    base_key = jax.random.fold_in(key, 21)
    base_draw = jnp.clip(jax.random.normal(base_key, (SEQ_LEN, KV_HEADS, HEAD_DIM), jnp.float32), -5.0, 5.0)
    return base_draw.reshape(SEQ_LEN, KV_HEADS * HEAD_DIM).astype(jnp.bfloat16)


def draw_queries(key, part):
    base_key = jax.random.fold_in(key, 31)
    group_size = HEADS // KV_HEADS
    shape_full = (SEQ_LEN, KV_HEADS, group_size, HEAD_DIM)
    base_draw = jnp.clip(1.5 * jax.random.normal(base_key, shape_full, jnp.float32), -5.0, 5.0)
    return base_draw.reshape(SEQ_LEN, HEADS * HEAD_DIM).astype(jnp.bfloat16)


def level_of(own_key, dims, pieces, low, high):
    factor_of = 1.0
    for axis_at, parts in pieces:
        draws = jax.random.uniform(jax.random.fold_in(jax.random.fold_in(own_key, 6), axis_at), (parts,), jnp.float32, low / len(pieces), high / len(pieces))
        factor_of = factor_of * jnp.repeat(jnp.exp(draws), dims[axis_at] // parts).reshape((-1,) + (1,) * (len(dims) - 1 - axis_at))
    return factor_of


def length_profile(amount, total, most, lean):
    portions = [(1 << 20) // math.isqrt(grade ** lean) + 1 for grade in range(2, amount + 1)]
    spare, counts = total - most - (amount - 1), [1] * (amount - 1)
    while spare > 0:
        movable = [i for i in range(amount - 1) if counts[i] < most]
        whole, remaining = sum([portions[i] for i in movable]), spare
        for i in movable:
            addition = min(most - counts[i], max(1, remaining * portions[i] // whole), spare)
            counts[i] = counts[i] + addition
            spare = spare - addition
    return np.array([most] + counts)


def uneven_parts(own_key, number_of, total, limit, slope):
    if number_of == 2:
        one = jax.random.randint(own_key, (), max(1, total - limit), min(limit, total - 1) + 1)
        return jnp.stack([one, total - one])
    sizes = jnp.asarray(length_profile(number_of, total, limit, slope), jnp.int32)
    pairs = (number_of - 1) // 2
    donor, receiver = sizes[1:1 + 2 * pairs:2], sizes[2:2 + 2 * pairs:2]
    margin = jnp.minimum(donor - 1, limit - receiver)
    moved = jax.random.randint(jax.random.fold_in(own_key, 1), (pairs,), 0, 1 << 20) % (margin + 1)
    sizes = sizes.at[1:1 + 2 * pairs:2].set(donor - moved).at[2:2 + 2 * pairs:2].set(receiver + moved)
    return sizes[jax.random.permutation(jax.random.fold_in(own_key, 2), number_of)]


def noise(own_key, extent, deviation, most, pieces=(), kind=jnp.bfloat16):
    gain = level_of(own_key, extent, pieces, -0.22, 0.18) if pieces else 1.0
    values = jax.random.normal(own_key, extent, jnp.float32) * deviation * gain
    return jnp.minimum(jnp.maximum(values, -most), most).astype(kind)


def setup_inputs(seed: int = 0, part: int = 0) -> dict:
    key_list = jax.random.split(jax.random.key(seed), 5)
    part_keys = jax.random.split(jax.random.fold_in(key_list[4], part), 5)
    queries = draw_queries(jax.random.fold_in(jax.random.fold_in(key_list[4], part), 71), part)
    keys = draw_keys(jax.random.fold_in(jax.random.fold_in(key_list[4], part), 71), part)
    values = noise(part_keys[2], (SEQ_LEN, KV_HEADS * HEAD_DIM), 1.0, 6.0, ((0, 16),))
    doc_lengths = uneven_parts(part_keys[3], DOCS, SEQ_LEN, MOST_DOC, 1).astype(jnp.int32)
    return {"queries": queries, "keys": keys, "values": values, "doc_lengths": doc_lengths}


rope_base = 1000000.0
negative = -1.0e30


def doc_place(position, doc_lengths):
    doc_ends = jnp.cumsum(doc_lengths).astype(jnp.int32)
    beyond = position[:, None] >= doc_ends[None, :]
    doc_index = jnp.sum(beyond.astype(jnp.int32), axis=1).astype(jnp.int32)
    doc_start = jnp.sum(jnp.where(beyond, doc_lengths[None, :], 0), axis=1).astype(jnp.int32)
    return doc_index, doc_start


def rotate(values_in, within_doc, head_count):
    row_count = values_in.shape[0]
    half_dim = HEAD_DIM // 2
    inverse_freq = jnp.power(jnp.float32(rope_base), -2.0 * jnp.arange(half_dim, dtype=jnp.float32) / HEAD_DIM)
    angles = within_doc.astype(jnp.float32)[:, None] * inverse_freq[None, :]
    cosine = jnp.cos(angles)[:, None, :]
    sines = jnp.sin(angles)[:, None, :]
    fields = values_in.astype(jnp.float32).reshape(row_count, head_count, HEAD_DIM)
    lower_half = fields[..., :half_dim]
    upper_half = fields[..., half_dim:]
    rotated = jnp.concatenate([lower_half * cosine - upper_half * sines, upper_half * cosine + lower_half * sines], axis=-1)
    return rotated.reshape(row_count, head_count * HEAD_DIM).astype(jnp.bfloat16)


def reference(queries, keys, values, doc_lengths):
    seq_total = queries.shape[0]
    group_size = HEADS // KV_HEADS
    score_scale = HEAD_DIM ** -0.5
    position = jnp.arange(seq_total, dtype=jnp.int32)
    doc_index, doc_start = doc_place(position, doc_lengths)
    within_doc = position - doc_start
    q_rot = rotate(queries, within_doc, HEADS)
    k_rot = rotate(keys, within_doc, KV_HEADS)
    k_heads = k_rot.reshape(seq_total, KV_HEADS, HEAD_DIM).astype(jnp.float32)
    v_heads = values.reshape(seq_total, KV_HEADS, HEAD_DIM).astype(jnp.float32)
    block_rows = min(512, seq_total)
    q_blocks = q_rot.reshape(seq_total // block_rows, block_rows, KV_HEADS, group_size, HEAD_DIM)
    pos_blocks = position.reshape(-1, block_rows)
    doc_blocks = doc_index.reshape(-1, block_rows)

    def attend_block(packed_in):
        q_block, pos_block, doc_block = packed_in
        scores = jnp.einsum("qkgd,skd->qkgs", q_block.astype(jnp.float32), k_heads) * score_scale
        allowed = (doc_index[None, :] == doc_block[:, None]) & (position[None, :] <= pos_block[:, None])
        allowed = allowed[:, None, None, :]
        scores = jnp.where(allowed, scores, negative)
        row_max = jnp.max(scores, axis=-1, keepdims=True)
        weight = jnp.where(allowed, jnp.exp(scores - row_max), 0.0)
        weight_sum = jnp.sum(weight, axis=-1)
        weight_b = lax.optimization_barrier(weight.astype(jnp.bfloat16))
        mixed_out = jnp.einsum("qkgs,skd->qkgd", weight_b.astype(jnp.float32), v_heads)
        mixed_out = mixed_out / weight_sum[..., None]
        return mixed_out.reshape(block_rows, HEADS * HEAD_DIM).astype(jnp.bfloat16)

    attended = lax.map(attend_block, (q_blocks, pos_blocks, doc_blocks))
    return attended.reshape(seq_total, HEADS * HEAD_DIM)
```

```python
import functools
import math

import jax
import jax.numpy as jnp
import numpy as np
from jax import lax
from jax.experimental import pallas as pl
from jax.experimental.pallas import tpu as pltpu
from jax.sharding import PartitionSpec as P

HEADS = 28
KV_HEADS = 4
HEAD_DIM = 128
GROUP = HEADS // KV_HEADS
HALF = HEAD_DIM // 2
ROPE_BASE = 1000000.0
NEGATIVE = -1e30
LONGEST_NUM, LONGEST_DEN = 5, 8
QUAD = 4
MESH = pl.DeviceIdType.MESH
TURN = 2.0 * math.pi
TURN_HI = float(np.float32(6.28125))
TURN_LO = float(np.float32(TURN - 6.28125))


def sine_coefficients():
    nodes = np.cos(np.pi * (np.arange(400) + 0.5) / 400) * 0.5 + 0.5
    square = nodes * (math.pi * 1.001) ** 2
    root = np.sqrt(square)
    fit = np.polynomial.Polynomial.fit(square, np.sin(root) / root, 7).convert()
    return [float(c) for c in fit.coef]


SINE = sine_coefficients()


def starts_of(position, doc_ref, docs):
    end = jnp.int32(0)
    start = jnp.zeros_like(position)
    for i in range(docs):
        end = end + doc_ref[i]
        start = jnp.where(position >= end, end, start)
    return start


def sine_cosine(angle):
    turns = jnp.floor(angle * (1.0 / TURN) + 0.5)
    rest = (angle - turns * TURN_HI) - turns * TURN_LO
    lane = lax.broadcasted_iota(jnp.int32, angle.shape, 1)
    rest = rest + jnp.where(lane < HALF, 0.0, 0.5 * math.pi)
    rest = jnp.where(rest > math.pi, rest - TURN, rest)
    square = rest * rest
    total = jnp.full_like(square, SINE[-1])
    for c in SINE[-2::-1]:
        total = total * square + c
    return total * rest


def kernel(n, doc_ref, freq_ref, q_ref, k_ref, v_ref, out_ref,
           kbuf, vbuf, cos_t, sin_t, bias, qrot, krot, peak, wsum, acc,
           send_a, send_b, send_c, recv_a, recv_b, recv_c):
    rows = q_ref.shape[0]
    docs = doc_ref.shape[0]
    levels = n // QUAD
    window = (LONGEST_NUM * n * rows // LONGEST_DEN - 1 + rows - 1) // rows
    lags = kbuf.shape[0]
    span = QUAD * rows
    me = lax.axis_index("seq")
    z, q = me // QUAD, me % QUAD
    y, core = q // 2, q % 2
    q1 = y * 2 + (1 - core)
    q2 = (1 - y) * 2 + core
    q3 = (1 - y) * 2 + (1 - core)
    up, down, across, twin = me + QUAD, me - QUAD, z * QUAD + q2, z * QUAD + q1

    def need(b, d):
        return (b < d) & (d <= b + window)

    def have_a(lag):
        return (z >= lag) & ((z - lag) * QUAD + q + window >= z * QUAD)

    def give_a(lag):
        return (z + 1 < levels) & ((z - lag) * QUAD + q + window >= (z + 1) * QUAD) & (z >= lag)

    def moves_b(lag, source, target, beside):
        b, base = (z - lag) * QUAD + source, z * QUAD
        return (z >= lag) & (need(b, base + target) | need(b, base + beside))

    def moves_c(lag, source, target):
        return (z >= lag) & need((z - lag) * QUAD + source, z * QUAD + target)

    def copy_of(part, source, lag, slot, send, recv, where):
        buf = (kbuf, vbuf)[part]
        return pltpu.make_async_remote_copy(
            src_ref=source, dst_ref=buf.at[lag, slot], send_sem=send, recv_sem=recv,
            device_id={"seq": where}, device_id_type=MESH)

    def held(part, lag, slot):
        if lag == 0 and slot is q:
            return (k_ref, v_ref)[part]
        return (kbuf, vbuf)[part].at[lag, slot]

    def copy_a(part, lag):
        return copy_of(part, held(part, lag, q), lag + 1, q, send_a.at[lag, part], recv_a.at[lag + 1, part], up)

    def copy_b(part, lag):
        return copy_of(part, held(part, lag, q), lag, q, send_b.at[lag, part], recv_b.at[lag, part], across)

    def copy_c(part, lag, which):
        slot = (q, q2)[which]
        return copy_of(part, held(part, lag, slot), lag, slot, send_c.at[lag, which, part],
                       recv_c.at[lag, which, part], twin)

    def arrival(part, lag, slot, recv, sender):
        return copy_of(part, (kbuf, vbuf)[part].at[lag, slot], lag, slot, send_a.at[0, part], recv, sender)

    barrier = pltpu.get_barrier_semaphore()
    pl.semaphore_signal(barrier, inc=1, device_id={"seq": twin}, device_id_type=MESH)
    pl.semaphore_signal(barrier, inc=1, device_id={"seq": across}, device_id_type=MESH)

    @pl.when(z + 1 < levels)
    def _():
        pl.semaphore_signal(barrier, inc=1, device_id={"seq": up}, device_id_type=MESH)

    @pl.when(z > 0)
    def _():
        pl.semaphore_signal(barrier, inc=1, device_id={"seq": down}, device_id_type=MESH)

    pl.semaphore_wait(barrier, 2 + jnp.where(z > 0, 1, 0) + jnp.where(z + 1 < levels, 1, 0))

    def forward_a(lag):
        for part in range(2):
            if lag > 0:
                @pl.when(have_a(lag))
                def _(part=part):
                    arrival(part, lag, q, recv_a.at[lag, part], down).wait_recv()

            if lag + 1 < lags:
                @pl.when(give_a(lag))
                def _(part=part):
                    copy_a(part, lag).start()

            @pl.when(moves_b(lag, q, q2, q3))
            def _(part=part):
                copy_b(part, lag).start()

            @pl.when(moves_c(lag, q, q1))
            def _(part=part):
                copy_c(part, lag, 0).start()

    def forward_b(lag):
        for part in range(2):
            @pl.when(moves_b(lag, q2, q, q1))
            def _(part=part):
                arrival(part, lag, q2, recv_b.at[lag, part], across).wait_recv()

            @pl.when(moves_c(lag, q2, q1))
            def _(part=part):
                copy_c(part, lag, 1).start()

    def land_c(lag):
        for part in range(2):
            @pl.when(moves_c(lag, q1, q))
            def _(part=part):
                arrival(part, lag, q1, recv_c.at[lag, 0, part], twin).wait_recv()

            @pl.when(moves_c(lag, q3, q))
            def _(part=part):
                arrival(part, lag, q3, recv_c.at[lag, 1, part], twin).wait_recv()

    forward_a(0)

    freq = freq_ref[:1, :]
    row_pos = me * rows + lax.broadcasted_iota(jnp.int32, (rows, rows), 1)
    row_start = starts_of(row_pos, doc_ref, docs)
    lane = lax.broadcasted_iota(jnp.int32, (rows, HEAD_DIM), 1)

    def tables(lag, slot):
        first = ((z - lag) * QUAD + slot) * rows
        at = first + lax.broadcasted_iota(jnp.int32, (rows, HEAD_DIM), 0)
        within = (at - starts_of(at, doc_ref, docs)).astype(jnp.float32)
        both = sine_cosine(within * freq)
        turned = pltpu.roll(both, HALF, 1)
        cos_t[lag, slot] = jnp.where(lane < HALF, turned, both)
        sin_t[lag, slot] = jnp.where(lane < HALF, -both, turned)
        s = first + lax.broadcasted_iota(jnp.int32, (rows, rows), 0)
        allowed = (s <= row_pos) & (s >= row_start)
        bias[lag, slot] = jnp.where(allowed, 0.0, NEGATIVE)

    def rotated(x, lag, slot):
        x = x.astype(jnp.float32)
        return (x * cos_t[lag, slot] + pltpu.roll(x, HALF, 1) * sin_t[lag, slot]).astype(jnp.bfloat16)

    def low_slot(lag):
        return max(0, lag * QUAD - window)

    for lag in range(lags):
        @pl.when(z >= lag)
        def _(lag=lag):
            def one(slot, carry):
                tables(lag, slot)
                return carry

            lax.fori_loop(low_slot(lag), QUAD, one, 0)

            for slot, gets in ((q1, moves_c(lag, q1, q)), (q2, moves_b(lag, q2, q, q1)),
                               (q3, moves_c(lag, q3, q))) + (((q, have_a(lag)),) if lag else ()):
                @pl.when(jnp.logical_not(gets))
                def _(slot=slot):
                    kbuf[lag, slot] = jnp.zeros(kbuf.shape[2:], kbuf.dtype)
                    vbuf[lag, slot] = jnp.zeros(vbuf.shape[2:], vbuf.dtype)

    kbuf[0, q] = k_ref[...]
    vbuf[0, q] = v_ref[...]

    def turn_queries(h, carry):
        cols = pl.ds(pl.multiple_of(h * HEAD_DIM, HEAD_DIM), HEAD_DIM)
        qrot[h // GROUP, pl.ds(pl.multiple_of((h % GROUP) * rows, rows), rows), :] = rotated(q_ref[:, cols], 0, q)
        return carry

    lax.fori_loop(0, HEADS, turn_queries, 0)

    scale = HEAD_DIM ** -0.5 * math.log2(math.e)

    def attend(lag):
        low = low_slot(lag)
        keys = (QUAD - low) * rows

        def one(kv, carry):
            cols = pl.ds(pl.multiple_of(kv * HEAD_DIM, HEAD_DIM), HEAD_DIM)
            for slot in range(low, QUAD):
                krot[pl.ds((slot - low) * rows, rows), :] = rotated(kbuf[lag, slot, :, cols], lag, slot)
            scores = lax.dot_general(krot[pl.ds(0, keys), :], qrot[kv], (((1,), (1,)), ((), ())),
                                     preferred_element_type=jnp.float32)
            mask = bias[lag, low:].reshape(keys, rows)
            scores = scores + jnp.concatenate([mask] * GROUP, axis=1)
            top = jnp.max(scores, axis=0, keepdims=True)
            if lag > 0:
                old = peak[kv][:1]
                top = jnp.maximum(top, old)
            weight = jnp.exp2((scores - top) * scale)
            sums = jnp.sum(weight, axis=0, keepdims=True)
            vals = vbuf[lag, low:, :, cols].reshape(keys, HEAD_DIM)
            part = lax.dot_general(vals, weight.astype(jnp.bfloat16), (((0,), (0,)), ((), ())),
                                   preferred_element_type=jnp.float32)
            if lag > 0:
                shrink = jnp.exp2((old - top) * scale)
                sums = wsum[kv][:1] * shrink + sums
                part = acc[kv] * shrink + part
            peak[kv] = jnp.broadcast_to(top, peak.shape[1:])
            wsum[kv] = jnp.broadcast_to(sums, wsum.shape[1:])
            acc[kv] = part
            return carry

        lax.fori_loop(0, KV_HEADS, one, 0)

    for lag in range(lags + 1):
        if lag + 1 < lags:
            forward_a(lag + 1)
        if lag < lags:
            forward_b(lag)
            land_c(lag)

            if lag == 0:
                attend(0)
            else:
                @pl.when(z >= lag)
                def _(lag=lag):
                    attend(lag)

    def finish(kv, carry):
        result = acc[kv] / wsum[kv][:1]
        for g in range(GROUP):
            cols = pl.ds(pl.multiple_of((kv * GROUP + g) * HEAD_DIM, HEAD_DIM), HEAD_DIM)
            out_ref[:, cols] = result[:, g * rows:(g + 1) * rows].T.astype(out_ref.dtype)
        return carry

    lax.fori_loop(0, KV_HEADS, finish, 0)

    for lag in range(lags):
        for part in range(2):
            if lag + 1 < lags:
                @pl.when(give_a(lag))
                def _(lag=lag, part=part):
                    copy_a(part, lag).wait_send()

            @pl.when(moves_b(lag, q, q2, q3))
            def _(lag=lag, part=part):
                copy_b(part, lag).wait_send()

            @pl.when(moves_c(lag, q, q1))
            def _(lag=lag, part=part):
                copy_c(part, lag, 0).wait_send()

            @pl.when(moves_c(lag, q2, q1))
            def _(lag=lag, part=part):
                copy_c(part, lag, 1).wait_send()


def per_device(n, queries, keys, values, doc_lengths):
    rows, width = queries.shape
    kv_width = keys.shape[1]
    window = (LONGEST_NUM * n * rows // LONGEST_DEN - 1 + rows - 1) // rows
    lags = min(n // QUAD, (window + QUAD - 1) // QUAD + 1)
    freq = ROPE_BASE ** (-2.0 * (np.arange(HEAD_DIM) % HALF) / HEAD_DIM)
    freq = jnp.asarray(np.tile(freq.astype(np.float32)[None, :], (8, 1)))
    vmem = pl.BlockSpec(memory_space=pltpu.VMEM)
    dma = pltpu.SemaphoreType.DMA
    return pl.pallas_call(
        functools.partial(kernel, n),
        out_shape=jax.ShapeDtypeStruct((rows, width), jnp.bfloat16),
        in_specs=[pl.BlockSpec(memory_space=pltpu.SMEM), vmem, vmem, vmem, vmem],
        out_specs=vmem,
        scratch_shapes=[
            pltpu.VMEM((lags, QUAD, rows, kv_width), jnp.bfloat16),
            pltpu.VMEM((lags, QUAD, rows, kv_width), jnp.bfloat16),
            pltpu.VMEM((lags, QUAD, rows, HEAD_DIM), jnp.float32),
            pltpu.VMEM((lags, QUAD, rows, HEAD_DIM), jnp.float32),
            pltpu.VMEM((lags, QUAD, rows, rows), jnp.float32),
            pltpu.VMEM((KV_HEADS, GROUP * rows, HEAD_DIM), jnp.bfloat16),
            pltpu.VMEM((QUAD * rows, HEAD_DIM), jnp.bfloat16),
            pltpu.VMEM((KV_HEADS, 8, GROUP * rows), jnp.float32),
            pltpu.VMEM((KV_HEADS, 8, GROUP * rows), jnp.float32),
            pltpu.VMEM((KV_HEADS, HEAD_DIM, GROUP * rows), jnp.float32),
            dma((lags, 2)), dma((lags, 2)), dma((lags, 2, 2)),
            dma((lags, 2)), dma((lags, 2)), dma((lags, 2, 2)),
        ],
        compiler_params=pltpu.CompilerParams(
            collective_id=0, has_side_effects=True, vmem_limit_bytes=60 * 1024 * 1024
        ),
    )(doc_lengths, freq, queries, keys, values)


def solution(mesh):
    return jax.shard_map(
        functools.partial(per_device, mesh.shape["seq"]),
        mesh=mesh,
        in_specs=(
            P(("grp", "seq"), None),
            P(("grp", "seq"), None),
            P(("grp", "seq"), None),
            P("grp"),
        ),
        out_specs=P(("grp", "seq"), None),
        check_vma=False,
    )
```

```python
import functools
import math

import jax
import jax.numpy as jnp
import numpy as np
from jax import lax
from jax.experimental import pallas as pl
from jax.experimental.pallas import tpu as pltpu
from jax.sharding import PartitionSpec as P

HEADS = 28
KV_HEADS = 4
HEAD_DIM = 128
GROUP = HEADS // KV_HEADS
HALF = HEAD_DIM // 2
ROPE_BASE = 1000000.0
NEGATIVE = -1e30
LONGEST_NUM, LONGEST_DEN = 5, 8
QUAD = 4
CHUNKS = 2
PARTS = 2 * CHUNKS
MESH = pl.DeviceIdType.MESH
TURN = 2.0 * math.pi
TURN_HI = float(np.float32(6.28125))
TURN_LO = float(np.float32(TURN - 6.28125))


def sine_coefficients():
    nodes = np.cos(np.pi * (np.arange(400) + 0.5) / 400) * 0.5 + 0.5
    square = nodes * (math.pi * 1.001) ** 2
    root = np.sqrt(square)
    fit = np.polynomial.Polynomial.fit(square, np.sin(root) / root, 7).convert()
    return [float(c) for c in fit.coef]


SINE = sine_coefficients()


def starts_of(position, doc_ref, docs):
    end = jnp.int32(0)
    start = jnp.zeros_like(position)
    for i in range(docs):
        end = end + doc_ref[i]
        start = jnp.where(position >= end, end, start)
    return start


def sine_cosine(angle):
    turns = jnp.floor(angle * (1.0 / TURN) + 0.5)
    rest = (angle - turns * TURN_HI) - turns * TURN_LO
    lane = lax.broadcasted_iota(jnp.int32, angle.shape, 1)
    rest = rest + jnp.where(lane < HALF, 0.0, 0.5 * math.pi)
    rest = jnp.where(rest > math.pi, rest - TURN, rest)
    square = rest * rest
    total = jnp.full_like(square, SINE[-1])
    for c in SINE[-2::-1]:
        total = total * square + c
    return total * rest


def kernel(n, doc_ref, freq_ref, q_ref, k_ref, v_ref, out_ref,
           kbuf, vbuf, cos_t, sin_t, bias, qrot, krot, peak, wsum, acc,
           send_a, send_b, send_c, send_far, recv_a, recv_b, recv_c):
    rows = q_ref.shape[0]
    docs = doc_ref.shape[0]
    levels = n // QUAD
    window = (LONGEST_NUM * n * rows // LONGEST_DEN - 1 + rows - 1) // rows
    lags = kbuf.shape[0]
    direct = False
    far = lags - 1
    relay_lags = lags - 1 if direct else lags
    wide = k_ref.shape[1] // CHUNKS
    span = QUAD * rows
    me = lax.axis_index("seq")
    z, q = me // QUAD, me % QUAD
    y, core = q // 2, q % 2
    q1 = y * 2 + (1 - core)
    q2 = (1 - y) * 2 + core
    q3 = (1 - y) * 2 + (1 - core)
    up, down, across, twin = me + QUAD, me - QUAD, z * QUAD + q2, z * QUAD + q1

    def need(b, d):
        return (b < d) & (d <= b + window)

    def have_a(lag):
        return (z >= lag) & ((z - lag) * QUAD + q + window >= z * QUAD)

    def give_a(lag):
        return (z + 1 < levels) & ((z - lag) * QUAD + q + window >= (z + 1) * QUAD) & (z >= lag)

    def moves_b(lag, source, target, beside):
        b, base = (z - lag) * QUAD + source, z * QUAD
        return (z >= lag) & (need(b, base + target) | need(b, base + beside))

    def moves_c(lag, source, target):
        return (z >= lag) & need((z - lag) * QUAD + source, z * QUAD + target)

    def place(part, lag, slot):
        cols = pl.ds(part // 2 * wide, wide)
        return (kbuf, vbuf)[part % 2].at[lag, slot, :, cols]

    def copy_of(part, source, lag, slot, send, recv, where):
        return pltpu.make_async_remote_copy(
            src_ref=source, dst_ref=place(part, lag, slot), send_sem=send, recv_sem=recv,
            device_id={"seq": where}, device_id_type=MESH)

    def held(part, lag, slot):
        if lag == 0 and slot is q:
            return (k_ref, v_ref)[part % 2].at[:, pl.ds(part // 2 * wide, wide)]
        return place(part, lag, slot)

    def copy_a(part, lag):
        return copy_of(part, held(part, lag, q), lag + 1, q, send_a.at[lag, part], recv_a.at[lag + 1, part], up)

    def copy_b(part, lag):
        return copy_of(part, held(part, lag, q), lag, q, send_b.at[lag, part], recv_b.at[lag, part], across)

    def copy_c(part, lag, which):
        slot = (q, q2)[which]
        return copy_of(part, held(part, lag, slot), lag, slot, send_c.at[lag, which, part],
                       recv_c.at[lag, which, part], twin)

    gives_far = (q >= 2) & (z + far < levels) & (
        need(me, me + far * QUAD - 2) | need(me, (z + far) * QUAD + q3))
    takes_far = (q < 2) & moves_b(far, q2, q, q1)

    def copy_far(part):
        return copy_of(part, held(part, 0, q), far, q, send_far.at[part], recv_b.at[far, part],
                       (z + far) * QUAD + q2)

    def arrival(part, lag, slot, recv, sender):
        return copy_of(part, place(part, lag, slot), lag, slot, send_a.at[0, part], recv, sender)

    barrier = pltpu.get_barrier_semaphore()
    pl.semaphore_signal(barrier, inc=1, device_id={"seq": twin}, device_id_type=MESH)
    pl.semaphore_signal(barrier, inc=1, device_id={"seq": across}, device_id_type=MESH)

    @pl.when(z + 1 < levels)
    def _():
        pl.semaphore_signal(barrier, inc=1, device_id={"seq": up}, device_id_type=MESH)

    @pl.when(z > 0)
    def _():
        pl.semaphore_signal(barrier, inc=1, device_id={"seq": down}, device_id_type=MESH)

    extra = 0
    if direct:
        @pl.when(gives_far)
        def _():
            pl.semaphore_signal(barrier, inc=1, device_id={"seq": (z + far) * QUAD + q2}, device_id_type=MESH)

        @pl.when(takes_far)
        def _():
            pl.semaphore_signal(barrier, inc=1, device_id={"seq": (z - far) * QUAD + q2}, device_id_type=MESH)

        extra = jnp.where(gives_far, 1, 0) + jnp.where(takes_far, 1, 0)

    pl.semaphore_wait(barrier, 2 + extra + jnp.where(z > 0, 1, 0) + jnp.where(z + 1 < levels, 1, 0))

    def forward_a(lag, chunk):
        for part in (2 * chunk, 2 * chunk + 1):
            if lag > 0:
                @pl.when(have_a(lag))
                def _(part=part):
                    arrival(part, lag, q, recv_a.at[lag, part], down).wait_recv()

            if lag + 1 < relay_lags:
                @pl.when(give_a(lag))
                def _(part=part):
                    copy_a(part, lag).start()

            @pl.when(moves_b(lag, q, q2, q3))
            def _(part=part):
                copy_b(part, lag).start()

            @pl.when(moves_c(lag, q, q1))
            def _(part=part):
                copy_c(part, lag, 0).start()

    def gets_b(lag):
        return takes_far if direct and lag == far else moves_b(lag, q2, q, q1)

    def forward_b(lag, chunk):
        for part in (2 * chunk, 2 * chunk + 1):
            @pl.when(gets_b(lag))
            def _(part=part):
                arrival(part, lag, q2, recv_b.at[lag, part], across).wait_recv()

            @pl.when(moves_c(lag, q2, q1))
            def _(part=part):
                copy_c(part, lag, 1).start()

    def land_c(lag, chunk):
        for part in (2 * chunk, 2 * chunk + 1):
            if not (direct and lag == far):
                @pl.when(moves_c(lag, q1, q))
                def _(part=part):
                    arrival(part, lag, q1, recv_c.at[lag, 0, part], twin).wait_recv()

            @pl.when(moves_c(lag, q3, q))
            def _(part=part):
                arrival(part, lag, q3, recv_c.at[lag, 1, part], twin).wait_recv()

    for chunk in range(CHUNKS):
        forward_a(0, chunk)
    if direct:
        @pl.when(gives_far)
        def _():
            for part in range(PARTS):
                copy_far(part).start()

    freq = freq_ref[:1, :]
    row_pos = me * rows + lax.broadcasted_iota(jnp.int32, (rows, rows), 1)
    row_start = starts_of(row_pos, doc_ref, docs)
    lane = lax.broadcasted_iota(jnp.int32, (rows, HEAD_DIM), 1)

    def tables(lag, slot):
        first = ((z - lag) * QUAD + slot) * rows
        at = first + lax.broadcasted_iota(jnp.int32, (rows, HEAD_DIM), 0)
        within = (at - starts_of(at, doc_ref, docs)).astype(jnp.float32)
        both = sine_cosine(within * freq)
        turned = pltpu.roll(both, HALF, 1)
        cos_t[lag, slot] = jnp.where(lane < HALF, turned, both)
        sin_t[lag, slot] = jnp.where(lane < HALF, -both, turned)
        s = first + lax.broadcasted_iota(jnp.int32, (rows, rows), 0)
        allowed = (s <= row_pos) & (s >= row_start)
        bias[lag, slot] = jnp.where(allowed, 0.0, NEGATIVE)

    def rotated(x, lag, slot):
        x = x.astype(jnp.float32)
        return (x * cos_t[lag, slot] + pltpu.roll(x, HALF, 1) * sin_t[lag, slot]).astype(jnp.bfloat16)

    def low_slot(lag):
        return max(0, lag * QUAD - window)

    for lag in range(lags):
        @pl.when(z >= lag)
        def _(lag=lag):
            def one(slot, carry):
                tables(lag, slot)
                return carry

            lax.fori_loop(low_slot(lag), QUAD, one, 0)

            for slot, gets in ((q1, moves_c(lag, q1, q)), (q2, moves_b(lag, q2, q, q1)),
                               (q3, moves_c(lag, q3, q))) + (((q, have_a(lag)),) if lag else ()):
                @pl.when(jnp.logical_not(gets))
                def _(slot=slot):
                    kbuf[lag, slot] = jnp.zeros(kbuf.shape[2:], kbuf.dtype)
                    vbuf[lag, slot] = jnp.zeros(vbuf.shape[2:], vbuf.dtype)

    kbuf[0, q] = k_ref[...]
    vbuf[0, q] = v_ref[...]

    def turn_queries(h, carry):
        cols = pl.ds(pl.multiple_of(h * HEAD_DIM, HEAD_DIM), HEAD_DIM)
        qrot[h // GROUP, pl.ds(pl.multiple_of((h % GROUP) * rows, rows), rows), :] = rotated(q_ref[:, cols], 0, q)
        return carry

    lax.fori_loop(0, HEADS, turn_queries, 0)

    scale = HEAD_DIM ** -0.5 * math.log2(math.e)

    def attend(lag, chunk):
        low = low_slot(lag)
        keys = (QUAD - low) * rows

        def one(kv, carry):
            cols = pl.ds(pl.multiple_of(kv * HEAD_DIM, HEAD_DIM), HEAD_DIM)
            for slot in range(low, QUAD):
                krot[pl.ds((slot - low) * rows, rows), :] = rotated(kbuf[lag, slot, :, cols], lag, slot)
            scores = lax.dot_general(krot[pl.ds(0, keys), :], qrot[kv], (((1,), (1,)), ((), ())),
                                     preferred_element_type=jnp.float32)
            mask = bias[lag, low:].reshape(keys, rows)
            scores = scores + jnp.concatenate([mask] * GROUP, axis=1)
            top = jnp.max(scores, axis=0, keepdims=True)
            if lag > 0:
                old = peak[kv][:1]
                top = jnp.maximum(top, old)
            weight = jnp.exp2((scores - top) * scale)
            sums = jnp.sum(weight, axis=0, keepdims=True)
            vals = vbuf[lag, low:, :, cols].reshape(keys, HEAD_DIM)
            part = lax.dot_general(vals, weight.astype(jnp.bfloat16), (((0,), (0,)), ((), ())),
                                   preferred_element_type=jnp.float32)
            if lag > 0:
                shrink = jnp.exp2((old - top) * scale)
                sums = wsum[kv][:1] * shrink + sums
                part = acc[kv] * shrink + part
            peak[kv] = jnp.broadcast_to(top, peak.shape[1:])
            wsum[kv] = jnp.broadcast_to(sums, wsum.shape[1:])
            acc[kv] = part
            return carry

        lax.fori_loop(chunk * KV_HEADS // CHUNKS, (chunk + 1) * KV_HEADS // CHUNKS, one, 0, unroll=True)

    order = list(range(lags))
    if direct:
        order = order[:-2] + [far, far - 1]
    for step, lag in enumerate(order):
        for chunk in range(CHUNKS):
            if step + 1 < relay_lags:
                forward_a(step + 1, chunk)
            forward_b(lag, chunk)
            land_c(lag, chunk)

            @pl.when((z >= lag) & ((z - lag) * QUAD + QUAD - 1 + window >= me))
            def _(lag=lag, chunk=chunk):
                attend(lag, chunk)

    def finish(kv, carry):
        result = acc[kv] / wsum[kv][:1]
        for g in range(GROUP):
            cols = pl.ds(pl.multiple_of((kv * GROUP + g) * HEAD_DIM, HEAD_DIM), HEAD_DIM)
            out_ref[:, cols] = result[:, g * rows:(g + 1) * rows].T.astype(out_ref.dtype)
        return carry

    lax.fori_loop(0, KV_HEADS, finish, 0)

    for part in range(PARTS):
        if direct:
            @pl.when(gives_far)
            def _(part=part):
                copy_far(part).wait_send()

        for lag in range(lags):
            if lag + 1 < relay_lags:
                @pl.when(give_a(lag))
                def _(lag=lag, part=part):
                    copy_a(part, lag).wait_send()

            if lag < relay_lags:
                @pl.when(moves_b(lag, q, q2, q3))
                def _(lag=lag, part=part):
                    copy_b(part, lag).wait_send()

                @pl.when(moves_c(lag, q, q1))
                def _(lag=lag, part=part):
                    copy_c(part, lag, 0).wait_send()

            @pl.when(moves_c(lag, q2, q1))
            def _(lag=lag, part=part):
                copy_c(part, lag, 1).wait_send()


def per_device(n, queries, keys, values, doc_lengths):
    rows, width = queries.shape
    kv_width = keys.shape[1]
    window = (LONGEST_NUM * n * rows // LONGEST_DEN - 1 + rows - 1) // rows
    lags = min(n // QUAD, (window + QUAD - 1) // QUAD + 1)
    freq = ROPE_BASE ** (-2.0 * (np.arange(HEAD_DIM) % HALF) / HEAD_DIM)
    freq = jnp.asarray(np.tile(freq.astype(np.float32)[None, :], (8, 1)))
    vmem = pl.BlockSpec(memory_space=pltpu.VMEM)
    dma = pltpu.SemaphoreType.DMA
    return pl.pallas_call(
        functools.partial(kernel, n),
        out_shape=jax.ShapeDtypeStruct((rows, width), jnp.bfloat16),
        in_specs=[pl.BlockSpec(memory_space=pltpu.SMEM), vmem, vmem, vmem, vmem],
        out_specs=vmem,
        scratch_shapes=[
            pltpu.VMEM((lags, QUAD, rows, kv_width), jnp.bfloat16),
            pltpu.VMEM((lags, QUAD, rows, kv_width), jnp.bfloat16),
            pltpu.VMEM((lags, QUAD, rows, HEAD_DIM), jnp.float32),
            pltpu.VMEM((lags, QUAD, rows, HEAD_DIM), jnp.float32),
            pltpu.VMEM((lags, QUAD, rows, rows), jnp.float32),
            pltpu.VMEM((KV_HEADS, GROUP * rows, HEAD_DIM), jnp.bfloat16),
            pltpu.VMEM((QUAD * rows, HEAD_DIM), jnp.bfloat16),
            pltpu.VMEM((KV_HEADS, 8, GROUP * rows), jnp.float32),
            pltpu.VMEM((KV_HEADS, 8, GROUP * rows), jnp.float32),
            pltpu.VMEM((KV_HEADS, HEAD_DIM, GROUP * rows), jnp.float32),
            dma((lags, PARTS)), dma((lags, PARTS)), dma((lags, 2, PARTS)), dma((PARTS,)),
            dma((lags, PARTS)), dma((lags, PARTS)), dma((lags, 2, PARTS)),
        ],
        compiler_params=pltpu.CompilerParams(
            collective_id=0, has_side_effects=True, vmem_limit_bytes=60 * 1024 * 1024
        ),
    )(doc_lengths, freq, queries, keys, values)


def solution(mesh):
    return jax.shard_map(
        functools.partial(per_device, mesh.shape["seq"]),
        mesh=mesh,
        in_specs=(
            P(("grp", "seq"), None),
            P(("grp", "seq"), None),
            P(("grp", "seq"), None),
            P("grp"),
        ),
        out_specs=P(("grp", "seq"), None),
        check_vma=False,
    )
```
